32 devices in a mesh: row: 8 (over z, x), col: 4 (over y, core).
Axes of the slice: x: 2, y: 2, z: 4, core: 2. Of those that a mesh axis runs over, the one named last changes fastest.
Arguments:
- gradients: bfloat16 [32, 1024, 5120], P(('row', 'col')), may hold values from -24 to 24
- bucket_lengths: int32 [16], replicated, may hold values from 1 to 128, 1024 in all
- owner_offset: int32 [8], replicated, may hold values from 0 to 3
- clip_rms: float32 [1], replicated, may hold values from 0.15 to 0.4
Outputs:
- clipped_shard: float32 [1024, 5120], P('row', 'col')
- bucket_rms: float32 [16], replicated
The draws below stay inside these ranges and needn't reach their ends.
Inputs may be any that keep to these rules, and one draw needn't show every extreme that they name: `bucket_lengths`: the buckets cover all 1024 rows; the largest has exactly 128 rows.
All inputs are finite; a program needn't handle non-finite values.
Results may differ from the reference program's by a relative error of at most 0.0003.
Values sent between devices are 32-bit elements; how exact they have to be, the bound alone decides.
A program may use at most 128 MiB of HBM per device.

```python
import math
import jax
import jax.numpy as jnp
import numpy as np
from jax import lax

D = 5120
ROWS = 1024
NBUCK = 16
MOSTB = 128
N_ROW = 8
N_COL = 4


def draw_gradients(key, part):
    devices = N_ROW * N_COL
    noise_key = jax.random.fold_in(key, 11)
    scale_key = jax.random.fold_in(key, 12)
    row_scale = jnp.exp(jax.random.uniform(scale_key, (ROWS,), jnp.float32, jnp.log(0.25), jnp.log(4.0)))
    noise = jax.random.normal(noise_key, (devices, ROWS, D), jnp.float32)
    values = 4.0 * row_scale[None, :, None] * noise
    return jnp.clip(values, -24.0, 24.0).astype(jnp.bfloat16)


def set_ends(result, stream_key, smallest, largest):
    extent = result.shape
    spot = [jax.random.randint(jax.random.fold_in(stream_key, axis), (), 0, extent[axis]) for axis in range(len(extent))]
    result = result.at[tuple(spot)].set(smallest)
    longest = extent.index(max(extent))
    spot[longest] = (spot[longest] + 1) % extent[longest]
    return result.at[tuple(spot)].set(largest)


def profile(count, total, limit, lean):
    portions = [(1 << 20) // math.isqrt(grade ** lean) + 1 for grade in range(2, count + 1)]
    rest, counts = total - limit - (count - 1), [1] * (count - 1)
    while rest > 0:
        movable = [i for i in range(count - 1) if counts[i] < limit]
        pool, budget = sum([portions[i] for i in movable]), rest
        for i in movable:
            extra = min(limit - counts[i], max(1, budget * portions[i] // pool), rest)
            counts[i] = counts[i] + extra
            rest = rest - extra
    return np.array([limit] + counts)


def uneven_parts(stream_key, amount, total, reach, lean):
    if amount == 2:
        one = jax.random.randint(stream_key, (), max(1, total - reach), min(reach, total - 1) + 1)
        return jnp.stack([one, total - one])
    lengths = jnp.asarray(profile(amount, total, reach, lean), jnp.int32)
    couples = (amount - 1) // 2
    source_of, receiver = lengths[1:1 + 2 * couples:2], lengths[2:2 + 2 * couples:2]
    slack = jnp.minimum(source_of - 1, reach - receiver)
    shifted = jax.random.randint(jax.random.fold_in(stream_key, 1), (couples,), 0, 1 << 20) % (slack + 1)
    lengths = lengths.at[1:1 + 2 * couples:2].set(source_of - shifted).at[2:2 + 2 * couples:2].set(receiver + shifted)
    return lengths[jax.random.permutation(jax.random.fold_in(stream_key, 2), amount)]


def setup_inputs(seed: int = 0) -> dict:
    keys = jax.random.split(jax.random.key(seed), 5)
    return {
        "gradients": draw_gradients(jax.random.fold_in(keys[4], 71), 0),
        "bucket_lengths": uneven_parts(keys[1], NBUCK, ROWS, MOSTB, 2).astype(jnp.int32),
        "owner_offset": set_ends(jax.random.randint(keys[2], (N_ROW,), 0, N_COL), jax.random.fold_in(keys[2], 1), 0, N_COL - 1).astype(jnp.int32),
        "clip_rms": jnp.clip(jax.random.uniform(keys[3], (1,), jnp.float32, 0.15, 0.4), 0.15, 0.4),
    }


def reference(gradients, bucket_lengths, owner_offset, clip_rms):
    devices = N_ROW * N_COL

    def accumulate(index, total):
        return total + gradients[index].astype(jnp.float32)
    summed = lax.fori_loop(0, devices, accumulate, jnp.zeros((ROWS, D), jnp.float32))
    averaged = summed / devices
    ends = jnp.cumsum(bucket_lengths).astype(jnp.int32)
    starts = (ends - bucket_lengths).astype(jnp.int32)
    row_ids = jnp.arange(ROWS, dtype=jnp.int32)
    member = ((row_ids[:, None] >= starts[None, :]) & (row_ids[:, None] < ends[None, :])).astype(jnp.float32)
    row_squares = lax.optimization_barrier(jnp.sum(averaged * averaged, axis=1))
    bucket_squares = lax.optimization_barrier(jnp.sum(row_squares[:, None] * member, axis=0))
    overall = jnp.sqrt(jnp.sum(bucket_squares) / (ROWS * D))
    factor = clip_rms[0] / jnp.maximum(overall, clip_rms[0])
    clipped = (averaged * factor).reshape(N_ROW, ROWS // N_ROW, D)
    shifts = (owner_offset * (D // N_COL)).astype(jnp.int32)

    def turn(block, shift):
        return jnp.roll(block, -shift, axis=1)
    clipped_shard = jax.vmap(turn)(clipped, shifts).reshape(ROWS, D)
    bucket_rms = jnp.sqrt(bucket_squares / (bucket_lengths.astype(jnp.float32) * D))
    return (clipped_shard, bucket_rms)
```

```python
import functools

import jax
import jax.numpy as jnp
from jax import lax
from jax.experimental import pallas as pl
from jax.experimental.pallas import tpu as pltpu
from jax.sharding import PartitionSpec as P

MESH = pl.DeviceIdType.MESH
F32 = jnp.float32


def kernel(
    n_row, n_col, g_ref, bounds_ref, pick_ref, clip_ref, avg_ref, fac_ref, rms_ref,
    src, send0, recv0, recv1, recv2, recv3, mine, slots, sq,
    load_sem, s0, r0, s1, r1, s2, r2, s3, r3, sa, ra,
):
    steps = recv0.shape[0]
    depth = n_row // 2
    devices = n_row * n_col
    total_rows, width = src.shape
    rows, w = total_rows // n_row, width // n_col
    row, col = lax.axis_index("row"), lax.axis_index("col")
    z, x = row // 2, row % 2
    y, core = col // 2, col % 2
    me = row * n_col + col
    core_peer = (row, y * 2 + 1 - core)
    peers = ((z * 2 + 1 - x, col), (row, (1 - y) * 2 + core))

    def place(k):
        other = (me + k) % devices
        return (other // n_col, other % n_col)

    def load(i):
        part = pl.ds(pl.multiple_of(i * rows, 16), rows)
        return pltpu.make_async_copy(g_ref.at[0, part], src.at[part], load_sem.at[i])

    def remote(a, b, s, r, dev):
        return pltpu.make_async_remote_copy(
            src_ref=a, dst_ref=b, send_sem=s, recv_sem=r, device_id=dev, device_id_type=MESH
        )

    def copy0(t, o):
        return remote(send0.at[t, o], recv0.at[t, o], s0.at[t, o], r0.at[t, o], core_peer)

    def copy1(t, o):
        return remote(recv0.at[t, o, 1], recv1.at[t, o], s1.at[t, o], r1.at[t, o], peers[o])

    def copy2(t, o):
        return remote(recv1.at[t, o, 1], recv2.at[t, o], s2.at[t, o], r2.at[t, o], peers[1 - o])

    def copy3(t, o, k):
        other = (z + k) % depth
        return remote(
            recv2.at[t, o, other], recv3.at[t, o, k - 1], s3.at[t, o, k - 1], r3.at[t, o, k - 1],
            (other * 2 + x, col),
        )

    def copya(k):
        return remote(mine, slots.at[me], sa.at[k], ra.at[me], place(k))

    for i in range(n_row):
        load(i).start()
    barrier = pltpu.get_barrier_semaphore()

    @pl.loop(1, devices)
    def _(k):
        pl.semaphore_signal(barrier, inc=1, device_id=place(k), device_id_type=MESH)

    pl.semaphore_wait(barrier, devices - 1)
    for i in range(n_row):
        load(i).wait()

    def piece(t, xr, yr, zi, to):
        r = zi * 2 + (x + xr) % 2
        c = ((y + yr) % 2) * 2 + to
        at = pl.ds(pl.multiple_of(r * rows + t * 16, 16), 16)
        total = None
        for j in range(n_col):
            weight = jnp.full((16, w), pick_ref[(r * n_col + c) * n_col + j], F32)
            term = src[at, j * w:(j + 1) * w] * weight.astype(src.dtype)
            total = term if total is None else total + term
        return total.astype(F32)

    def convert(t):
        for xr in (1, 0):
            for yr in (1, 0):
                @pl.loop(0, depth)
                def _(zi):
                    v = piece(t, xr, yr, zi, 1 - core)
                    send0[t, 0, xr, yr, zi] = v[:8]
                    send0[t, 1, yr, xr, zi] = v[8:]
        for o in range(2):
            copy0(t, o).start()

    def stage0(t):
        for o in range(2):
            copy0(t, o).wait_recv()
        for xr in (1, 0):
            for yr in (1, 0):
                @pl.loop(0, depth)
                def _(zi):
                    v = piece(t, xr, yr, zi, core)
                    recv0[t, 0, xr, yr, zi] += v[:8]
                    recv0[t, 1, yr, xr, zi] += v[8:]
        for o in range(2):
            copy1(t, o).start()

    def stage1(t):
        for o in range(2):
            copy1(t, o).wait_recv()
            for d in (1, 0):
                @pl.loop(0, depth)
                def _(zi):
                    recv1[t, o, d, zi] += recv0[t, o, 0, d, zi]
            copy2(t, o).start()

    def stage2(t):
        for o in range(2):
            copy2(t, o).wait_recv()

            @pl.loop(0, depth)
            def _(zi):
                recv2[t, o, zi] += recv1[t, o, 0, zi]

            for k in range(1, depth):
                copy3(t, o, k).start()

    def stage3(t):
        for o in range(2):
            v = recv2[t, o, z]
            for k in range(1, depth):
                copy3(t, o, k).wait_recv()
                v = v + recv3[t, o, k - 1]
            v = v * (1.0 / devices)
            at = pl.ds(pl.multiple_of(t * 16 + o * 8, 8), 8)
            avg_ref[at, :] = v
            v = v * v
            part = v[:, 0:128]
            for j in range(128, w, 128):
                part = part + v[:, j:j + 128]
            sq[at, :] = part

    stages = (convert, stage0, stage1, stage2, stage3)

    @pl.loop(0, steps + len(stages) - 1)
    def _(t):
        for lag, stage in enumerate(stages):
            @pl.when((t >= lag) & (t < steps + lag))
            def _():
                stage(t - lag)

    ids = lax.broadcasted_iota(jnp.int32, (rows, 128), 0) + row * rows
    starts, ends = bounds_ref[0:1, :], bounds_ref[1:2, :]
    after = jnp.clip(ids - starts + 1, 0, 1)
    before = jnp.clip(ends - ids, 0, 1)
    inside = (after * before).astype(F32)
    row_squares = jnp.sum(sq[...], axis=1, keepdims=True)
    local = jnp.sum(inside * row_squares, axis=0, keepdims=True)
    mine[...] = jnp.broadcast_to(local, mine.shape)
    slots[me] = jnp.broadcast_to(local, mine.shape)

    @pl.loop(1, devices)
    def _(k):
        copya(k).start()

    @pl.loop(0, steps)
    def _(t):
        for o in range(2):
            copy0(t, o).wait_send()
            copy1(t, o).wait_send()
            copy2(t, o).wait_send()
            for k in range(1, depth):
                copy3(t, o, k).wait_send()

    @pl.loop(1, devices)
    def _(k):
        other = (me + devices - k) % devices
        remote(mine, slots.at[other], sa.at[k], ra.at[other], place(k)).wait_recv()
        copya(k).wait_send()

    squares = lax.fori_loop(
        0, devices, lambda i, a: a + slots[i], jnp.zeros(mine.shape, F32)
    )
    overall = jnp.sqrt(jnp.sum(squares, axis=1, keepdims=True) / (total_rows * width))
    clip = clip_ref[0]
    fac_ref[...] = jnp.broadcast_to(clip / jnp.maximum(overall, clip), fac_ref.shape)
    safe = jnp.maximum(ends - starts, 1).astype(F32) * width
    rms_ref[...] = jnp.sqrt(squares / safe)


def shards(n_row, n_col, gradients, bucket_lengths, owner_offset, clip_rms):
    _, total_rows, width = gradients.shape
    rows, w = total_rows // n_row, width // n_col
    devices = n_row * n_col
    steps, depth = rows // 16, n_row // 2
    vmem, smem = pltpu.VMEM, pltpu.SMEM
    dma = pltpu.SemaphoreType.DMA
    ends = jnp.cumsum(bucket_lengths)
    bounds = jnp.stack([ends - bucket_lengths, ends])
    bounds = jnp.pad(bounds, ((0, 6), (0, 128 - bucket_lengths.shape[0])))
    block = jnp.arange(n_col, dtype=jnp.int32)
    origin = (block[None, :] + owner_offset[:, None]) % n_col
    pick = (origin[:, :, None] == block[None, None, :]).astype(F32).reshape(-1)
    averaged, factor, rms = pl.pallas_call(
        functools.partial(kernel, n_row, n_col),
        out_shape=(
            jax.ShapeDtypeStruct((rows, w), F32),
            jax.ShapeDtypeStruct((8, 128), F32),
            jax.ShapeDtypeStruct((8, 128), F32),
        ),
        in_specs=[
            pl.BlockSpec(memory_space=pl.ANY),
            pl.BlockSpec(memory_space=vmem),
            pl.BlockSpec(memory_space=smem),
            pl.BlockSpec(memory_space=smem),
        ],
        out_specs=[pl.BlockSpec(memory_space=vmem)] * 3,
        scratch_shapes=[
            vmem((total_rows, width), gradients.dtype),
            vmem((steps, 2, 2, 2, depth, 8, w), F32),
            vmem((steps, 2, 2, 2, depth, 8, w), F32),
            vmem((steps, 2, 2, depth, 8, w), F32),
            vmem((steps, 2, depth, 8, w), F32),
            vmem((steps, 2, depth - 1, 8, w), F32),
            vmem((8, 128), F32),
            vmem((devices, 8, 128), F32),
            vmem((rows, 128), F32),
            dma((n_row,)),
            dma((steps, 2)), dma((steps, 2)),
            dma((steps, 2)), dma((steps, 2)),
            dma((steps, 2)), dma((steps, 2)),
            dma((steps, 2, depth - 1)), dma((steps, 2, depth - 1)),
            dma((devices,)), dma((devices,)),
        ],
        compiler_params=pltpu.CompilerParams(
            collective_id=0, has_side_effects=True, vmem_limit_bytes=60 * 1024 * 1024
        ),
    )(gradients, bounds, pick, clip_rms)
    return averaged * factor[0, 0], rms[0, : bucket_lengths.shape[0]]


def solution(mesh):
    n_row, n_col = mesh.shape["row"], mesh.shape["col"]
    in_specs = (P(("row", "col"), None, None), P(), P(), P())
    out_specs = (P("row", "col"), P())
    return jax.shard_map(
        functools.partial(shards, n_row, n_col),
        mesh=mesh, in_specs=in_specs, out_specs=out_specs, check_vma=False,
    )
```

```python
import functools

import jax
import jax.numpy as jnp
from jax import lax
from jax.experimental import pallas as pl
from jax.experimental.pallas import tpu as pltpu
from jax.sharding import PartitionSpec as P

MESH = pl.DeviceIdType.MESH
F32 = jnp.float32
PARTS = 2
LAG = 2
ROWS = 16


def kernel(n_row, n_col, bits, g_ref, len_ref, off_ref, clip_ref, out_ref, rms_ref, src, send0, *rest):
    sums, rest = rest[: bits + 1], rest[bits + 1 :]
    mine, slots, sq, load_sem, sends, recvs, sa, ra = rest
    steps = send0.shape[0]
    blocks = 1 << bits
    devices = n_row * n_col
    _, rows, width = src.shape
    w = width // n_col
    part = w // PARTS
    row, col = lax.axis_index("row"), lax.axis_index("col")
    z, x = row // 2, row % 2
    y, core = col // 2, col % 2
    me = row * n_col + col

    def flip(value, bit):
        return value + (1 - 2 * ((value >> bit) % 2)) * (1 << bit)

    x_peer, y_peer = (flip(row, 0), col), (row, flip(col, 1))
    z_peers = [(flip(row, 1 + b), col) for b in range(bits - 2)]
    order = (
        [(row, flip(col, 0)), x_peer, z_peers[0], y_peer] + z_peers[1:],
        [(row, flip(col, 0)), y_peer, z_peers[0], x_peer] + z_peers[1:],
    )

    def place(k):
        other = (me + k) % devices
        return (other // n_col, other % n_col)

    def load(i):
        at = pl.ds(pl.multiple_of(i * ROWS, ROWS), ROWS)
        return pltpu.make_async_copy(g_ref.at[:, at], src.at[:, at], load_sem.at[i])

    def remote(a, b, s, r, dev):
        return pltpu.make_async_remote_copy(
            src_ref=a, dst_ref=b, send_sem=s, recv_sem=r, device_id=dev, device_id_type=MESH
        )

    def copy(stage, t, o):
        half = blocks >> stage
        a = send0.at[t, o] if stage == 0 else sums[stage - 1].at[t, o, pl.ds(half, half)]
        return remote(
            a, sums[stage].at[t, o], sends.at[stage, t, o], recvs.at[stage, t, o], order[o][stage]
        )

    def copya(k):
        return remote(mine, slots.at[me], sa.at[k], ra.at[me], place(k))

    @pl.loop(0, rows // ROWS)
    def _(i):
        load(i).start()

    barrier = pltpu.get_barrier_semaphore()

    @pl.loop(1, devices)
    def _(k):
        pl.semaphore_signal(barrier, inc=1, device_id=place(k), device_id_type=MESH)

    pl.semaphore_wait(barrier, devices - 1)

    def spot(i):
        xr, zr, yr = i >> (bits - 1), (i >> (bits - 2)) % 2, (i >> (bits - 3)) % 2
        low = i % (1 << (bits - 3))
        other = (
            (yr << (bits - 1)) + (zr << (bits - 2)) + (xr << (bits - 3)) + low
        )
        zd = (z + zr) % 2
        for b in range(1, bits - 2):
            zd = zd + ((((z >> b) + (low >> (bits - 3 - b))) % 2) << b)
        return zd * 2 + (x + xr) % 2, (y + yr) % 2, other

    def piece(t, r, c):
        at = pl.ds(pl.multiple_of((t // PARTS) * ROWS, ROWS), ROWS)
        origin = lax.rem(c + off_ref[r], n_col)
        total = None
        for j in range(n_col):
            gap = origin - j
            weight = jnp.maximum(1 - gap * gap, 0).astype(F32)
            begin = pl.multiple_of(j * w + (t % PARTS) * part, 128)
            term = src[r, at, pl.ds(begin, part)] * jnp.full((ROWS, part), weight, F32).astype(src.dtype)
            total = term if total is None else total + term
        return total.astype(F32)

    def convert(t):
        @pl.when(t % PARTS == 0)
        def _():
            load(t // PARTS).wait()

        @pl.loop(0, blocks)
        def _(i):
            r, yd, other = spot(i)
            v = piece(t, r, yd * 2 + 1 - core)
            send0[t, 0, i] = v[:8]
            send0[t, 1, other] = v[8:]

        for o in range(2):
            copy(0, t, o).start()

    def stage0(t):
        for o in range(2):
            copy(0, t, o).wait_recv()

        @pl.loop(0, blocks)
        def _(i):
            r, yd, other = spot(i)
            v = piece(t, r, yd * 2 + core)
            sums[0][t, 0, i] += v[:8]
            sums[0][t, 1, other] += v[8:]

        for o in range(2):
            copy(1, t, o).start()

    def fold(stage, t):
        for o in range(2):
            copy(stage, t, o).wait_recv()

            @pl.loop(0, blocks >> stage)
            def _(i):
                sums[stage][t, o, i] += sums[stage - 1][t, o, i]

            copy(stage + 1, t, o).start()

    def finish(t):
        for o in range(2):
            copy(bits, t, o).wait_recv()
            v = (sums[bits][t, o, 0] + sums[bits - 1][t, o, 0]) * (1.0 / devices)
            at = pl.ds(pl.multiple_of((t // PARTS) * ROWS + o * 8, 8), 8)
            out_ref[at, pl.ds(pl.multiple_of((t % PARTS) * part, 128), part)] = v
            v = v * v
            total = v[:, 0:128]
            for j in range(128, part, 128):
                total = total + v[:, j : j + 128]
            sq[t % PARTS, at, :] = total

    stages = [convert, stage0]
    stages += [functools.partial(fold, s) for s in range(1, bits)]
    stages += [finish]

    @pl.loop(0, steps + LAG * (len(stages) - 1))
    def _(t):
        for i, stage in enumerate(stages):
            lag = i * LAG

            @pl.when((t >= lag) & (t < steps + lag))
            def _():
                stage(t - lag)

    lane = lax.broadcasted_iota(jnp.int32, (1, 128), 1)
    starts = jnp.zeros((1, 128), jnp.int32)
    lengths = jnp.zeros((1, 128), jnp.int32)
    begin = jnp.int32(0)
    for b in range(len_ref.shape[0]):
        starts = jnp.where(lane == b, begin, starts)
        lengths = jnp.where(lane == b, len_ref[b], lengths)
        begin = begin + len_ref[b]
    ids = lax.broadcasted_iota(jnp.int32, (rows, 128), 0) + row * rows
    after = jnp.clip(ids - starts + 1, 0, 1)
    before = jnp.clip(starts + lengths - ids, 0, 1)
    inside = (after * before).astype(F32)
    row_squares = jnp.sum(jnp.sum(sq[...], axis=0), axis=1, keepdims=True)
    local = jnp.sum(inside * row_squares, axis=0, keepdims=True)
    mine[...] = local
    slots[me] = local

    @pl.loop(1, devices)
    def _(k):
        copya(k).start()

    @pl.loop(0, steps)
    def _(t):
        for o in range(2):
            for s in range(bits + 1):
                copy(s, t, o).wait_send()

    @pl.loop(1, devices)
    def _(k):
        other = (me + devices - k) % devices
        remote(mine, slots.at[other], sa.at[k], ra.at[other], place(k)).wait_recv()
        copya(k).wait_send()

    squares = slots[0]
    for i in range(1, devices):
        squares = squares + slots[i]
    overall = jnp.sqrt(jnp.sum(squares, axis=1, keepdims=True) / (n_row * rows * width))
    clip = clip_ref[0]
    factor = clip / jnp.maximum(overall, clip)
    out_ref[...] = out_ref[...] * factor
    rms = jnp.sqrt(squares / (jnp.maximum(lengths, 1).astype(F32) * width))
    rms_ref[...] = rms[:, : rms_ref.shape[1]]


def shards(n_row, n_col, gradients, bucket_lengths, owner_offset, clip_rms):
    _, total_rows, width = gradients.shape
    rows, w = total_rows // n_row, width // n_col
    devices = n_row * n_col
    steps = rows // ROWS * PARTS
    bits = devices.bit_length() - 2
    blocks = 1 << bits
    vmem, smem = pltpu.VMEM, pltpu.SMEM
    dma = pltpu.SemaphoreType.DMA
    clipped, rms = pl.pallas_call(
        functools.partial(kernel, n_row, n_col, bits),
        out_shape=(
            jax.ShapeDtypeStruct((rows, w), F32),
            jax.ShapeDtypeStruct((1, bucket_lengths.shape[0]), F32),
        ),
        in_specs=[
            pl.BlockSpec(memory_space=pl.ANY),
            pl.BlockSpec(memory_space=smem),
            pl.BlockSpec(memory_space=smem),
            pl.BlockSpec(memory_space=smem),
        ],
        out_specs=[pl.BlockSpec(memory_space=vmem)] * 2,
        scratch_shapes=[
            vmem((n_row, rows, width), gradients.dtype),
            vmem((steps, 2, blocks, 8, w // PARTS), F32),
            *[vmem((steps, 2, blocks >> s, 8, w // PARTS), F32) for s in range(bits + 1)],
            vmem((1, 128), F32),
            vmem((devices, 1, 128), F32),
            vmem((PARTS, rows, 128), F32),
            dma((rows // ROWS,)),
            dma((bits + 1, steps, 2)), dma((bits + 1, steps, 2)),
            dma((devices,)), dma((devices,)),
        ],
        compiler_params=pltpu.CompilerParams(
            collective_id=0, has_side_effects=True, vmem_limit_bytes=60 * 1024 * 1024
        ),
    )(gradients.reshape(n_row, rows, width), bucket_lengths, owner_offset, clip_rms)
    return clipped, rms[0]


def solution(mesh):
    n_row, n_col = mesh.shape["row"], mesh.shape["col"]
    in_specs = (P(("row", "col"), None, None), P(), P(), P())
    out_specs = (P("row", "col"), P())
    return jax.shard_map(
        functools.partial(shards, n_row, n_col),
        mesh=mesh, in_specs=in_specs, out_specs=out_specs, check_vma=False,
    )
```

```python
import functools

import jax
import jax.numpy as jnp
from jax import lax
from jax.experimental import pallas as pl
from jax.experimental.pallas import tpu as pltpu
from jax.sharding import PartitionSpec as P

MESH = pl.DeviceIdType.MESH
F32 = jnp.float32
PARTS = 2
LAG = 2
ROWS = 16


def kernel(n_row, n_col, bits, g_ref, len_ref, off_ref, clip_ref, out_ref, rms_ref, src, send0, *rest):
    sums, rest = rest[: bits + 1], rest[bits + 1 :]
    mine, slots, sq, load_sem, sends, recvs, sa, ra = rest
    steps = send0.shape[0]
    blocks = 1 << bits
    devices = n_row * n_col
    _, rows, width = src.shape
    w = width // n_col
    part = w // PARTS
    row, col = lax.axis_index("row"), lax.axis_index("col")
    z, x = row // 2, row % 2
    y, core = col // 2, col % 2
    me = row * n_col + col

    def flip(value, bit):
        return value + (1 - 2 * ((value >> bit) % 2)) * (1 << bit)

    x_peer, y_peer = (flip(row, 0), col), (row, flip(col, 1))
    z_peers = [(flip(row, 1 + b), col) for b in range(bits - 2)]
    order = (
        [(row, flip(col, 0)), x_peer, z_peers[0], y_peer] + z_peers[1:],
        [(row, flip(col, 0)), y_peer, z_peers[0], x_peer] + z_peers[1:],
    )

    def place(k):
        other = (me + k) % devices
        return (other // n_col, other % n_col)

    def load(i):
        at = pl.ds(pl.multiple_of(i * ROWS, ROWS), ROWS)
        return pltpu.make_async_copy(g_ref.at[:, at], src.at[:, at], load_sem.at[i])

    def remote(a, b, s, r, dev):
        return pltpu.make_async_remote_copy(
            src_ref=a, dst_ref=b, send_sem=s, recv_sem=r, device_id=dev, device_id_type=MESH
        )

    def copy(stage, t, o):
        half = blocks >> stage
        a = send0.at[t, o] if stage == 0 else sums[stage - 1].at[t, o, pl.ds(half, half)]
        return remote(
            a, sums[stage].at[t, o], sends.at[stage, t, o], recvs.at[stage, t, o], order[o][stage]
        )

    def copya(k):
        return remote(mine, slots.at[me], sa.at[k], ra.at[me], place(k))

    @pl.loop(0, rows // ROWS)
    def _(i):
        load(i).start()

    barrier = pltpu.get_barrier_semaphore()

    @pl.loop(1, devices)
    def _(k):
        pl.semaphore_signal(barrier, inc=1, device_id=place(k), device_id_type=MESH)

    pl.semaphore_wait(barrier, devices - 1)

    def spot(i):
        xr, zr, yr = i >> (bits - 1), (i >> (bits - 2)) % 2, (i >> (bits - 3)) % 2
        low = i % (1 << (bits - 3))
        other = (
            (yr << (bits - 1)) + (zr << (bits - 2)) + (xr << (bits - 3)) + low
        )
        zd = (z + zr) % 2
        for b in range(1, bits - 2):
            zd = zd + ((((z >> b) + (low >> (bits - 3 - b))) % 2) << b)
        return zd * 2 + (x + xr) % 2, (y + yr) % 2, other

    def piece(t, r, c):
        at = pl.ds(pl.multiple_of((t // PARTS) * ROWS, ROWS), ROWS)
        origin = lax.rem(c + off_ref[r], n_col)
        total = None
        for j in range(n_col):
            gap = origin - j
            weight = jnp.maximum(1 - gap * gap, 0).astype(F32)
            begin = pl.multiple_of(j * w + (t % PARTS) * part, 128)
            term = src[r, at, pl.ds(begin, part)] * jnp.full((ROWS, part), weight, F32).astype(src.dtype)
            total = term if total is None else total + term
        return total.astype(F32)

    def convert(t):
        @pl.when(t % PARTS == 0)
        def _():
            load(t // PARTS).wait()

        @pl.loop(0, blocks, unroll=2)
        def _(i):
            r, yd, other = spot(i)
            v = piece(t, r, yd * 2 + 1 - core)
            send0[t, 0, i] = v[:8]
            send0[t, 1, other] = v[8:]

        for o in range(2):
            copy(0, t, o).start()

    def stage0(t):
        for o in range(2):
            copy(0, t, o).wait_recv()

        @pl.loop(0, blocks, unroll=2)
        def _(i):
            r, yd, other = spot(i)
            v = piece(t, r, yd * 2 + core)
            sums[0][t, 0, i] += v[:8]
            sums[0][t, 1, other] += v[8:]

        for o in range(2):
            copy(1, t, o).start()

    def fold(stage, t):
        for o in range(2):
            copy(stage, t, o).wait_recv()

            @pl.loop(0, blocks >> stage, unroll=2)
            def _(i):
                sums[stage][t, o, i] += sums[stage - 1][t, o, i]

            copy(stage + 1, t, o).start()

    def finish(t):
        for o in range(2):
            copy(bits, t, o).wait_recv()
            v = (sums[bits][t, o, 0] + sums[bits - 1][t, o, 0]) * (1.0 / devices)
            at = pl.ds(pl.multiple_of((t // PARTS) * ROWS + o * 8, 8), 8)
            out_ref[at, pl.ds(pl.multiple_of((t % PARTS) * part, 128), part)] = v
            v = v * v
            total = v[:, 0:128]
            for j in range(128, part, 128):
                total = total + v[:, j : j + 128]
            sq[t % PARTS, at, :] = total

    stages = [convert, stage0]
    stages += [functools.partial(fold, s) for s in range(1, bits)]
    stages += [finish]

    @pl.loop(0, steps + LAG * (len(stages) - 1))
    def _(t):
        for i, stage in enumerate(stages):
            lag = i * LAG

            @pl.when((t >= lag) & (t < steps + lag))
            def _():
                stage(t - lag)

    lane = lax.broadcasted_iota(jnp.int32, (1, 128), 1)
    starts = jnp.zeros((1, 128), jnp.int32)
    lengths = jnp.zeros((1, 128), jnp.int32)
    begin = jnp.int32(0)
    for b in range(len_ref.shape[0]):
        starts = jnp.where(lane == b, begin, starts)
        lengths = jnp.where(lane == b, len_ref[b], lengths)
        begin = begin + len_ref[b]
    ids = lax.broadcasted_iota(jnp.int32, (rows, 128), 0) + row * rows
    after = jnp.clip(ids - starts + 1, 0, 1)
    before = jnp.clip(starts + lengths - ids, 0, 1)
    inside = (after * before).astype(F32)
    row_squares = jnp.sum(jnp.sum(sq[...], axis=0), axis=1, keepdims=True)
    local = jnp.sum(inside * row_squares, axis=0, keepdims=True)
    mine[...] = local
    slots[me] = local

    @pl.loop(1, devices)
    def _(k):
        copya(k).start()

    @pl.loop(0, steps)
    def _(t):
        for o in range(2):
            for s in range(bits + 1):
                copy(s, t, o).wait_send()

    @pl.loop(1, devices)
    def _(k):
        other = (me + devices - k) % devices
        remote(mine, slots.at[other], sa.at[k], ra.at[other], place(k)).wait_recv()
        copya(k).wait_send()

    squares = slots[0]
    for i in range(1, devices):
        squares = squares + slots[i]
    overall = jnp.sqrt(jnp.sum(squares, axis=1, keepdims=True) / (n_row * rows * width))
    clip = clip_ref[0]
    factor = clip / jnp.maximum(overall, clip)
    out_ref[...] = out_ref[...] * factor
    rms = jnp.sqrt(squares / (jnp.maximum(lengths, 1).astype(F32) * width))
    rms_ref[...] = rms[:, : rms_ref.shape[1]]


def shards(n_row, n_col, gradients, bucket_lengths, owner_offset, clip_rms):
    _, total_rows, width = gradients.shape
    rows, w = total_rows // n_row, width // n_col
    devices = n_row * n_col
    steps = rows // ROWS * PARTS
    bits = devices.bit_length() - 2
    blocks = 1 << bits
    vmem, smem = pltpu.VMEM, pltpu.SMEM
    dma = pltpu.SemaphoreType.DMA
    clipped, rms = pl.pallas_call(
        functools.partial(kernel, n_row, n_col, bits),
        out_shape=(
            jax.ShapeDtypeStruct((rows, w), F32),
            jax.ShapeDtypeStruct((1, bucket_lengths.shape[0]), F32),
        ),
        in_specs=[
            pl.BlockSpec(memory_space=pl.ANY),
            pl.BlockSpec(memory_space=smem),
            pl.BlockSpec(memory_space=smem),
            pl.BlockSpec(memory_space=smem),
        ],
        out_specs=[pl.BlockSpec(memory_space=vmem)] * 2,
        scratch_shapes=[
            vmem((n_row, rows, width), gradients.dtype),
            vmem((steps, 2, blocks, 8, w // PARTS), F32),
            *[vmem((steps, 2, blocks >> s, 8, w // PARTS), F32) for s in range(bits + 1)],
            vmem((1, 128), F32),
            vmem((devices, 1, 128), F32),
            vmem((PARTS, rows, 128), F32),
            dma((rows // ROWS,)),
            dma((bits + 1, steps, 2)), dma((bits + 1, steps, 2)),
            dma((devices,)), dma((devices,)),
        ],
        compiler_params=pltpu.CompilerParams(
            collective_id=0, has_side_effects=True, vmem_limit_bytes=44 * 1024 * 1024
        ),
    )(gradients.reshape(n_row, rows, width), bucket_lengths, owner_offset, clip_rms)
    return clipped, rms[0]


def solution(mesh):
    n_row, n_col = mesh.shape["row"], mesh.shape["col"]
    in_specs = (P(("row", "col"), None, None), P(), P(), P())
    out_specs = (P("row", "col"), P())
    return jax.shard_map(
        functools.partial(shards, n_row, n_col),
        mesh=mesh, in_specs=in_specs, out_specs=out_specs, check_vma=False,
    )
```
